32 devices in a mesh: grp: 2 (over x), tile: 16 (over z, y, core).
Axes of the slice: x: 2, y: 2, z: 4, core: 2. Of those that a mesh axis runs over, the one named last changes fastest.
Arguments:
- habitat: int32 [32, 4, 512], P(('grp', 'tile')), parts along dimension 0, may hold values from 0 to 15
- table: float32 [16], replicated, may hold values from 0.25 to 2
- source_cell: int32 [512], P('grp'), parts along dimension 0, may hold values from 0 to 32767
- ground_cell: int32 [512], P('grp'), parts along dimension 0, may hold values from 0 to 32767
- start_potential: float32 [32, 4, 512, 256], P(('grp', 'tile')), parts along dimension 0, may hold values from -30 to 30
Outputs:
- potentials: float32 [32, 4, 512, 256], P(('grp', 'tile')), parts along dimension 0
- residual: float32 [32, 4, 512, 256], P(('grp', 'tile')), parts along dimension 0
- resistance: float32 [512], P('grp'), parts along dimension 0
The draws below stay inside these ranges and needn't reach their ends.
There are 2 independent parts, one for each index of `grp`. The reference program is written for one: setup_inputs(seed, part) draws one part's arguments, and reference() takes and returns one part's arrays. A program takes and returns all parts, laid end to end along the dimension named above; an argument that names none is the same for every part. Nothing has to cross between parts.
Inputs may be any that keep to these rules, and one draw needn't show every extreme that they name: `source_cell`: an index row * 1024 + column of the raster. `ground_cell`: an index row * 1024 + column of the raster.
All inputs are finite; a program needn't handle non-finite values.
Results may differ from the reference program's by a relative error of at most 0.00018.
Values sent between devices are 32-bit elements; how exact they have to be, the bound alone decides.
No kernel may reach another device: no remote copies, remote signals or barrier semaphores. Data moves between devices by JAX's collectives and lax.ppermute only.
A program may use at most 128 MiB of HBM per device.

```python
import math
import jax
import jax.numpy as jnp

CX = 4
CY = 512
R = 256
CLASSES = 16
ITERS = 2
BLOCKS = 16
NX = 32
NY = 1024


def draw_start_potential(key, part):
    base_key = jax.random.fold_in(jax.random.fold_in(key, 17), 0)
    block_rows = jnp.arange(BLOCKS) // 2
    raster_rows = block_rows[:, None] * CX + jnp.arange(CX)[None, :]
    ramp = jnp.exp(1.1513 * raster_rows.astype(jnp.float32) / max(NX - 1, 1))
    field = jax.random.normal(base_key, (BLOCKS, CX, CY, R), jnp.float32)
    return field * ramp[:, :, None, None]


def set_ends(result, rng, low, largest):
    longest = result.shape.index(max(result.shape))
    spots = []
    for shift in (0, 1):
        where = [jax.random.randint(jax.random.fold_in(rng, axis), (), 0, length) for axis, length in enumerate(result.shape)]
        where[longest] = (where[longest] + shift) % result.shape[longest]
        spots.append(tuple(where))
    return result.at[spots[0]].set(low).at[spots[1]].set(largest)


def setup_inputs(seed: int = 0, part: int = 0) -> dict:
    keys = jax.random.split(jax.random.key(seed), 6)
    part_splits = jax.random.split(jax.random.fold_in(keys[5], part), 6)
    habitat = set_ends(jax.random.randint(part_splits[0], (BLOCKS, CX, CY), 0, CLASSES), jax.random.fold_in(part_splits[0], 1), 0, CLASSES - 1).astype(jnp.int32)
    table = jnp.clip(jnp.exp(jax.random.uniform(keys[1], (CLASSES,), jnp.float32, math.log(0.25), math.log(2.0))), 0.25, 2.0)
    source_cell = set_ends(jax.random.randint(part_splits[2], (R,), 0, NX * NY), jax.random.fold_in(part_splits[2], 1), 0, (NX * NY) - 1).astype(jnp.int32)
    ground_cell = set_ends(jax.random.randint(part_splits[3], (R,), 0, NX * NY), jax.random.fold_in(part_splits[3], 1), 0, (NX * NY) - 1).astype(jnp.int32)
    start_potential = draw_start_potential(jax.random.fold_in(jax.random.fold_in(keys[5], part), 71), part)
    return dict(habitat=habitat, table=table, source_cell=source_cell, ground_cell=ground_cell, start_potential=start_potential)


def to_raster(blocks):
    block_count, rows_here, cols_here = blocks.shape[0], blocks.shape[1], blocks.shape[2]
    trailing = blocks.shape[3:]
    blocks_grid = blocks.reshape((block_count // 2, 2, rows_here, cols_here) + trailing)
    blocks_grid = jnp.swapaxes(blocks_grid, 1, 2)
    return blocks_grid.reshape((block_count // 2 * rows_here, 2 * cols_here) + trailing)


def to_blocks(raster, rows_here, cols_here):
    trailing = raster.shape[2:]
    blocks_grid = raster.reshape((raster.shape[0] // rows_here, rows_here, 2, cols_here) + trailing)
    blocks_grid = jnp.swapaxes(blocks_grid, 1, 2)
    return blocks_grid.reshape((raster.shape[0] // rows_here * 2, rows_here, cols_here) + trailing)


def reference(habitat, table, source_cell, ground_cell, start_potential):
    classes = to_raster(habitat)
    conduct = table[classes]
    row_count, col_count = classes.shape[0], classes.shape[1]
    padded = jnp.pad(conduct, 1)
    row_index = jnp.arange(row_count)[:, None]
    col_index = jnp.arange(col_count)[None, :]
    north_w = jnp.where(row_index > 0, 0.5 * (conduct + padded[:-2, 1:-1]), 0.0)
    south_w = jnp.where(row_index < row_count - 1, 0.5 * (conduct + padded[2:, 1:-1]), 0.0)
    west_w = jnp.where(col_index > 0, 0.5 * (conduct + padded[1:-1, :-2]), 0.0)
    east_w = jnp.where(col_index < col_count - 1, 0.5 * (conduct + padded[1:-1, 2:]), 0.0)
    cell_ids = (row_index * col_count + col_index).astype(jnp.int32)
    ground_mask = (cell_ids[:, :, None] == ground_cell[None, None, :]).astype(jnp.float32)
    diagonal = (north_w + south_w + west_w + east_w)[:, :, None] + ground_mask
    source_field = (cell_ids[:, :, None] == source_cell[None, None, :]).astype(jnp.float32)

    def operate(field):
        pad_field = jnp.pad(field, ((1, 1), (1, 1), (0, 0)))
        applied = diagonal * field - north_w[:, :, None] * pad_field[:-2, 1:-1]
        applied = applied - south_w[:, :, None] * pad_field[2:, 1:-1]
        applied = applied - west_w[:, :, None] * pad_field[1:-1, :-2]
        return applied - east_w[:, :, None] * pad_field[1:-1, 2:]

    potentials = to_raster(start_potential)
    residual = source_field - operate(potentials)
    direction = residual
    norm_now = jnp.sum(residual * residual, axis=(0, 1))
    for iteration in range(ITERS):
        applied = operate(direction)
        step_size = norm_now / jnp.sum(direction * applied, axis=(0, 1))
        potentials = potentials + step_size * direction
        residual = residual - step_size * applied
        if iteration + 1 < ITERS:
            norm_next = jnp.sum(residual * residual, axis=(0, 1))
            direction = residual + (norm_next / norm_now) * direction
            norm_now = norm_next
    flattened = potentials.reshape((row_count * col_count, potentials.shape[2]))
    columns = jnp.arange(potentials.shape[2], dtype=jnp.int32)
    resistance = flattened[source_cell, columns] - flattened[ground_cell, columns]
    rows_here, cols_here = habitat.shape[1], habitat.shape[2]
    return to_blocks(potentials, rows_here, cols_here), to_blocks(residual, rows_here, cols_here), resistance
```

```python
import functools

import jax
import jax.numpy as jnp
from jax import lax
from jax.experimental import pallas as pl
from jax.experimental.pallas import tpu as pltpu
from jax.sharding import PartitionSpec as P

LANES = 128
HALO = 8
PAD = 16
DEPTH = 3


def exchange(value, mask):
    pairs = [(i, i ^ mask) for i in range(lax.axis_size("tile"))]
    return lax.ppermute(value, "tile", pairs)


def forward(value):
    count = lax.axis_size("tile")
    pairs = []
    for i in range(count):
        target = i + 4 if (i // 2) % 2 == 0 else i - 4
        if 0 <= target < count:
            pairs.append((i, target))
    return lax.ppermute(value, "tile", pairs)


def total(value):
    count = lax.axis_size("tile")
    bit = 1
    while bit < count:
        if bit * 2 < count:
            first = exchange(value, bit)
            second = exchange(value, 2 * bit)
            third = exchange(value, 3 * bit)
            value = (value + first) + (second + third)
            bit *= 4
        else:
            value = value + exchange(value, bit)
            bit *= 2
    return value


def extended(own, from_y, from_z):
    return jnp.concatenate([from_z[::-1], own, from_y[:0:-1]], 0)


def krylov_kernel(flip, own, y1, y2, y3, z0, z1, z2, left, right, ws, we, src, gnd, *rest):
    out_r, out_w, out_z, sums, xs, rs, wsc = rest[-7:]
    rows, cols = own.shape[0], own.shape[1]
    wide = xs.shape[1]
    first = HALO
    last = wide - HALO
    mirror = flip[0]

    def natural(i):
        return i + mirror * (rows - 1 - 2 * i)

    for e, piece in ((0, z2), (1, z1), (2, z0), (7, y3), (8, y2), (9, y1)):
        xs[e, PAD : PAD + cols, :] = piece[...]
    for i in range(rows):
        xs[DEPTH + i, PAD : PAD + cols, :] = own[natural(i)]
    zero = jnp.zeros((HALO, LANES), jnp.float32)
    for e in range(xs.shape[0]):
        xs[e, HALO:PAD, :] = left[e]
        xs[e, PAD + cols : PAD + cols + HALO, :] = right[e]
        for field in (xs, rs, wsc):
            field[e, 0:HALO, :] = zero
            field[e, last:wide, :] = zero
    source = src[...]
    ground = gnd[...]

    def cells(e, start, n):
        return lax.broadcasted_iota(jnp.int32, (n, LANES), 0) + (e * wide + start)

    def apply(field, e, start, n, ids):
        stop = start + n
        mid = field[e, start:stop, :]
        acc = ws[e - 1, start:stop, :] * (mid - field[e - 1, start:stop, :])
        acc += ws[e, start:stop, :] * (mid - field[e + 1, start:stop, :])
        acc += we[e, start - 1 : stop - 1, :] * (mid - field[e, start - 1 : stop - 1, :])
        acc += we[e, start:stop, :] * (mid - field[e, start + 1 : stop + 1, :])
        return mid, acc + jnp.where(ids == ground, mid, 0.0)

    step = 24

    @pl.loop(1, rows + 2 * DEPTH - 1)
    def _(e):
        for start in range(first, last, step):
            n = min(step, last - start)
            ids = cells(e, start, n)
            _, image = apply(xs, e, start, n, ids)
            rs[e, start : start + n, :] = jnp.where(ids == source, 1.0, 0.0) - image

    @pl.loop(2, rows + 2 * DEPTH - 2)
    def _(e):
        for start in range(first, last, step):
            n = min(step, last - start)
            ids = cells(e, start, n)
            _, image = apply(rs, e, start, n, ids)
            wsc[e, start : start + n, :] = image

    step_own = 32

    def fold(v):
        return jnp.sum(v.reshape(v.shape[0] // 8, 8, LANES), axis=0)

    def last_phase(i, carry):
        e = i + DEPTH
        row = natural(i)
        carry = list(carry)
        for start in range(0, cols, step_own):
            here = slice(PAD + start, PAD + start + step_own)
            ids = cells(e, PAD + start, step_own)
            w, z = apply(wsc, e, PAD + start, step_own, ids)
            r = rs[e, here, :]
            x = xs[e, here, :]
            there = slice(start, start + step_own)
            out_r[row, there, :] = r
            out_w[row, there, :] = w
            out_z[row, there, :] = z
            sign = jnp.where(ids == source, 1.0, 0.0) - jnp.where(ids == ground, 1.0, 0.0)
            terms = (r * r, r * w, w * w, w * z, sign * x, sign * r, sign * w)
            carry = [c + fold(t) for c, t in zip(carry, terms)]
        return tuple(carry)

    start_sums = tuple(jnp.zeros((8, LANES), jnp.float32) for _ in range(7))
    done = lax.fori_loop(0, rows, last_phase, start_sums)
    for q in range(7):
        sums[q : q + 1, :] = jnp.sum(done[q], axis=0, keepdims=True)
    sums[7:8, :] = jnp.zeros((1, LANES), jnp.float32)


def krylov(chunk, flip, own, ys, zs, left, right, ws, we, src, gnd, previous):
    rows, cols, width = own.shape
    wide = cols + 2 * PAD
    deep = rows + 2 * DEPTH
    lane = lambda c: chunk
    vm = functools.partial(pl.BlockSpec, memory_space=pltpu.VMEM)
    at_chunk3 = lambda i: (0, 0, chunk)
    at_chunk2 = lambda i: (0, chunk)
    whole2 = vm((cols, LANES), lambda i: (0, 0))
    whole3 = vm((deep, wide, LANES), lambda i: (0, 0, 0))
    block = vm((rows, cols, LANES), at_chunk3)
    edge = vm((deep, HALO, LANES), at_chunk3)
    ident = vm((1, LANES), at_chunk2)
    in_specs = [pl.BlockSpec(memory_space=pltpu.SMEM), block] + [whole2] * 6
    in_specs += [edge, edge, whole3, whole3, ident, ident]
    operands = [flip, own, ys[1], ys[2], ys[3], zs[0], zs[1], zs[2], left, right, ws, we, src, gnd]
    aliases = {}
    if previous is not None:
        for q, p in enumerate(previous):
            aliases[len(operands)] = q
            operands.append(p)
            in_specs.append(pl.BlockSpec(memory_space=pl.ANY))
    full = jax.ShapeDtypeStruct((rows, cols, width), jnp.float32)
    return pl.pallas_call(
        krylov_kernel,
        grid=(1,),
        in_specs=in_specs,
        out_specs=[block, block, block, vm((8, LANES), lambda i: (0, 0))],
        out_shape=[full, full, full, jax.ShapeDtypeStruct((8, LANES), jnp.float32)],
        scratch_shapes=[pltpu.VMEM((deep, wide, LANES), jnp.float32)] * 3,
        input_output_aliases=aliases,
        compiler_params=pltpu.CompilerParams(vmem_limit_bytes=48 * 1024 * 1024),
        name="krylov",
    )(*operands)


def shards(habitat, table, source_cell, ground_cell, start_potential):
    rows, cols = habitat.shape[1], habitat.shape[2]
    width = start_potential.shape[3]
    chunks = width // LANES
    deep = rows + 2 * DEPTH
    wide = cols + 2 * PAD
    me = lax.axis_index("tile")
    count = lax.axis_size("tile")
    block_row = me // 2
    block_col = me % 2
    flip = block_row % 2
    own = start_potential[0]

    def mirrored(value):
        return jnp.where(flip == 0, value, value[::-1])

    def inner(value):
        return jnp.where(block_col == 0, value[:, cols - HALO :], value[:, :HALO])

    def piece(j, chunk):
        row = j + flip * (rows - 1 - 2 * j)
        size = (1, cols, LANES)
        return lax.dynamic_slice(own, (row, 0, chunk * LANES), size)[0]

    classes = mirrored(habitat[0])
    levels = jnp.arange(table.shape[0], dtype=jnp.int32)
    conduct = jnp.sum(
        jnp.where(classes[:, :, None] == levels[None, None, :], table[None, None, :], 0.0), axis=2
    )
    side_cond = exchange(inner(conduct), 1)
    side_own = exchange(mirrored(inner(own)), 1)

    zero_side = jnp.zeros_like(side_cond)
    blank = jnp.zeros((rows, PAD - HALO), jnp.float32)
    wide_cond = jnp.concatenate(
        [
            blank,
            jnp.where(block_col == 1, side_cond, zero_side),
            conduct,
            jnp.where(block_col == 0, side_cond, zero_side),
            blank,
        ],
        1,
    )
    y_cond = exchange(wide_cond, 2)
    y_side = exchange(side_own, 2)
    z_cond = forward(y_cond[:DEPTH])
    z_side = forward(y_side[:DEPTH])
    ys = [[exchange(piece(j, c), 2) for j in range(rows)] for c in range(chunks)]
    zs = [[forward(ys[c][j]) for j in range(DEPTH)] for c in range(chunks)]

    cond = extended(wide_cond, y_cond, z_cond)
    sides = extended(side_own, y_side, z_side)
    has_z = jnp.where(flip == 0, me >= 4, me < count - 4)
    level = jnp.arange(deep)[:, None]
    next_row = jnp.concatenate([cond[1:], jnp.zeros((1, wide), jnp.float32)], 0)
    next_col = jnp.concatenate([cond[:, 1:], jnp.zeros((deep, 1), jnp.float32)], 1)
    ws = jnp.where(has_z | (level >= DEPTH), 0.5 * (cond + next_row), 0.0)
    low = jnp.where(block_col == 0, PAD, HALO)
    high = jnp.where(block_col == 0, wide - HALO, wide - PAD)
    spot = jnp.arange(wide)[None, :]
    we = jnp.where((spot >= low) & (spot + 1 < high), 0.5 * (cond + next_col), 0.0)
    ws = jnp.broadcast_to(ws[:, :, None], (deep, wide, LANES))
    we = jnp.broadcast_to(we[:, :, None], (deep, wide, LANES))
    left = jnp.where(block_col == 1, sides, 0.0)
    right = jnp.where(block_col == 0, sides, 0.0)

    def located(cell):
        row = cell // (2 * cols) - block_row * rows + DEPTH
        row = jnp.where(flip == 0, row, deep - 1 - row)
        col = cell % (2 * cols) - block_col * cols + PAD
        inside = (row >= 0) & (row < deep) & (col >= HALO) & (col < wide - HALO)
        return jnp.where(inside, row * wide + col, -1)[None, :]

    src = located(source_cell)
    gnd = located(ground_cell)
    flag = flip.astype(jnp.int32)[None]

    fields = None
    sums = []
    for c in range(chunks):
        *fields, part = krylov(
            c, flag, own, ys[c], zs[c], left, right, ws, we, src, gnd, fields
        )
        sums.append(part)
    rr, rw, ww, wz, xd, rd, wd, _ = total(jnp.concatenate(sums, 1))
    a0 = rr / rw
    rr1 = rr + a0 * (a0 * ww - 2.0 * rw)
    grow = 1.0 + rr1 / rr
    curve = grow * (grow * rw - 2.0 * a0 * ww) + a0 * a0 * wz
    a1 = rr1 / curve
    p = a0 + a1 * grow
    q = a0 * a1
    r, w, z = fields
    potentials = own + p * r - q * w
    residual = r - p * w + q * z
    return (potentials[None], residual[None], xd + p * rd - q * wd)


def solution(mesh):
    placed = (
        P(("grp", "tile"), None, None),
        P(),
        P("grp"),
        P("grp"),
        P(("grp", "tile"), None, None, None),
    )
    return jax.shard_map(
        shards,
        mesh=mesh,
        in_specs=placed,
        out_specs=(
            P(("grp", "tile"), None, None, None),
            P(("grp", "tile"), None, None, None),
            P("grp"),
        ),
        check_vma=False,
    )
```

```python
import functools

import jax
import jax.numpy as jnp
from jax import lax
from jax.experimental import pallas as pl
from jax.experimental.pallas import tpu as pltpu
from jax.sharding import PartitionSpec as P

LANES = 128
HALO = 8
PAD = 16
DEPTH = 3


def exchange(value, mask):
    pairs = [(i, i ^ mask) for i in range(lax.axis_size("tile"))]
    return lax.ppermute(value, "tile", pairs)


def forward(value):
    count = lax.axis_size("tile")
    pairs = []
    for i in range(count):
        target = i + 4 if (i // 2) % 2 == 0 else i - 4
        if 0 <= target < count:
            pairs.append((i, target))
    return lax.ppermute(value, "tile", pairs)


def across(value):
    pairs = []
    for i in range(lax.axis_size("tile")):
        other = i - 2 if (i // 2) % 2 == 0 else i + 2
        if 0 <= other < lax.axis_size("tile"):
            pairs.append((i, other))
    return lax.ppermute(value, "tile", pairs)


def total(value):
    count = lax.axis_size("tile")
    bit = 1
    while bit < count:
        if bit * 2 < count:
            first = exchange(value, bit)
            second = exchange(value, 2 * bit)
            third = exchange(value, 3 * bit)
            value = (value + first) + (second + third)
            bit *= 4
        else:
            value = value + exchange(value, bit)
            bit *= 2
    return value


def extended(own, from_y, from_z):
    parts = [from_z[d - 1 : d] for d in range(DEPTH, 0, -1)]
    parts.append(own)
    top = own.shape[0]
    parts += [from_y[top - d : top - d + 1] for d in range(1, DEPTH + 1)]
    return jnp.concatenate(parts, 0)


def krylov_kernel(flip, own, y1, y2, y3, z0, z1, z2, left, right, ws, we, src, gnd, *rest):
    out_r, out_w, out_z, sums, xs, rs, wsc = rest[-7:]
    rows, cols = own.shape[0], own.shape[1]
    wide = xs.shape[1]
    first = HALO
    last = wide - HALO
    mirror = flip[0]

    def natural(i):
        return i + mirror * (rows - 1 - 2 * i)

    for e, piece in ((0, z2), (1, z1), (2, z0), (7, y3), (8, y2), (9, y1)):
        xs[e, PAD : PAD + cols, :] = piece[...]
    for i in range(rows):
        xs[DEPTH + i, PAD : PAD + cols, :] = own[natural(i)]
    zero = jnp.zeros((HALO, LANES), jnp.float32)
    for e in range(xs.shape[0]):
        xs[e, HALO:PAD, :] = left[e]
        xs[e, PAD + cols : PAD + cols + HALO, :] = right[e]
        for field in (xs, rs, wsc):
            field[e, 0:HALO, :] = zero
            field[e, last:wide, :] = zero
    source = src[...]
    ground = gnd[...]

    def cells(e, start, n):
        return lax.broadcasted_iota(jnp.int32, (n, LANES), 0) + (e * wide + start)

    def apply(field, e, start, n, ids):
        stop = start + n
        mid = field[e, start:stop, :]
        acc = ws[e - 1, start:stop, :] * (mid - field[e - 1, start:stop, :])
        acc += ws[e, start:stop, :] * (mid - field[e + 1, start:stop, :])
        acc += we[e, start - 1 : stop - 1, :] * (mid - field[e, start - 1 : stop - 1, :])
        acc += we[e, start:stop, :] * (mid - field[e, start + 1 : stop + 1, :])
        return mid, acc + jnp.where(ids == ground, mid, 0.0)

    step = 24

    @pl.loop(1, rows + 2 * DEPTH - 1)
    def _(e):
        for start in range(first, last, step):
            n = min(step, last - start)
            ids = cells(e, start, n)
            _, image = apply(xs, e, start, n, ids)
            rs[e, start : start + n, :] = jnp.where(ids == source, 1.0, 0.0) - image

    @pl.loop(2, rows + 2 * DEPTH - 2)
    def _(e):
        for start in range(first, last, step):
            n = min(step, last - start)
            ids = cells(e, start, n)
            _, image = apply(rs, e, start, n, ids)
            wsc[e, start : start + n, :] = image

    step_own = 32

    def fold(v):
        return jnp.sum(v.reshape(v.shape[0] // 8, 8, LANES), axis=0)

    def last_phase(i, carry):
        e = i + DEPTH
        row = natural(i)
        carry = list(carry)
        for start in range(0, cols, step_own):
            here = slice(PAD + start, PAD + start + step_own)
            ids = cells(e, PAD + start, step_own)
            w, z = apply(wsc, e, PAD + start, step_own, ids)
            r = rs[e, here, :]
            x = xs[e, here, :]
            there = slice(start, start + step_own)
            out_r[row, there, :] = r
            out_w[row, there, :] = w
            out_z[row, there, :] = z
            sign = jnp.where(ids == source, 1.0, 0.0) - jnp.where(ids == ground, 1.0, 0.0)
            terms = (r * r, r * w, w * w, w * z, sign * x, sign * r, sign * w)
            carry = [c + fold(t) for c, t in zip(carry, terms)]
        return tuple(carry)

    start_sums = tuple(jnp.zeros((8, LANES), jnp.float32) for _ in range(7))
    done = lax.fori_loop(0, rows, last_phase, start_sums)
    for q in range(7):
        sums[q : q + 1, :] = jnp.sum(done[q], axis=0, keepdims=True)
    sums[7:8, :] = jnp.zeros((1, LANES), jnp.float32)


def krylov(chunk, flip, own, ys, zs, left, right, ws, we, src, gnd, previous):
    rows, cols, width = own.shape
    wide = cols + 2 * PAD
    deep = rows + 2 * DEPTH
    lane = lambda c: chunk
    vm = functools.partial(pl.BlockSpec, memory_space=pltpu.VMEM)
    at_chunk3 = lambda i: (0, 0, chunk)
    at_chunk2 = lambda i: (0, chunk)
    whole2 = vm((cols, LANES), lambda i: (0, 0))
    whole3 = vm((deep, wide, LANES), lambda i: (0, 0, 0))
    block = vm((rows, cols, LANES), at_chunk3)
    edge = vm((deep, HALO, LANES), at_chunk3)
    ident = vm((1, LANES), at_chunk2)
    in_specs = [pl.BlockSpec(memory_space=pltpu.SMEM), block] + [whole2] * 6
    in_specs += [edge, edge, whole3, whole3, ident, ident]
    operands = [flip, own, ys[1], ys[2], ys[3], zs[0], zs[1], zs[2], left, right, ws, we, src, gnd]
    aliases = {}
    if previous is not None:
        for q, p in enumerate(previous):
            aliases[len(operands)] = q
            operands.append(p)
            in_specs.append(pl.BlockSpec(memory_space=pl.ANY))
    full = jax.ShapeDtypeStruct((rows, cols, width), jnp.float32)
    return pl.pallas_call(
        krylov_kernel,
        grid=(1,),
        in_specs=in_specs,
        out_specs=[block, block, block, vm((8, LANES), lambda i: (0, 0))],
        out_shape=[full, full, full, jax.ShapeDtypeStruct((8, LANES), jnp.float32)],
        scratch_shapes=[pltpu.VMEM((deep, wide, LANES), jnp.float32)] * 3,
        input_output_aliases=aliases,
        compiler_params=pltpu.CompilerParams(vmem_limit_bytes=48 * 1024 * 1024),
        name="krylov",
    )(*operands)


def shards(habitat, table, source_cell, ground_cell, start_potential):
    rows, cols = habitat.shape[1], habitat.shape[2]
    width = start_potential.shape[3]
    chunks = width // LANES
    deep = rows + 2 * DEPTH
    wide = cols + 2 * PAD
    me = lax.axis_index("tile")
    count = lax.axis_size("tile")
    block_row = me // 2
    block_col = me % 2
    flip = block_row % 2
    own = start_potential[0]

    def mirrored(value):
        picked = []
        for j in range(rows):
            other = rows - 1 - j
            picked.append(jnp.where(flip == 0, value[j : j + 1], value[other : other + 1]))
        return jnp.concatenate(picked, 0)

    def inner(value):
        return jnp.where(block_col == 0, value[:, cols - HALO :], value[:, :HALO])

    def piece(source, j, chunk):
        row = j + flip * (rows - 1 - 2 * j)
        size = (1, cols, LANES)
        return lax.dynamic_slice(source, (row, 0, chunk * LANES), size)[0]

    lead = piece(own, 0, 0)
    lead, later, habitat = lax.optimization_barrier((lead, own, habitat))
    lead = exchange(lead, 2)
    classes = mirrored(habitat[0])
    levels = jnp.arange(table.shape[0], dtype=jnp.int32)
    conduct = jnp.sum(
        jnp.where(classes[:, :, None] == levels[None, None, :], table[None, None, :], 0.0), axis=2
    )
    strip = mirrored(inner(later))
    conduct, strip, last = lax.optimization_barrier((conduct, strip, later))
    cond_own = extended(conduct, exchange(conduct, 2), across(conduct))
    strips = extended(strip, exchange(strip, 2), across(strip))
    ys = [
        [lead if (j, c) == (0, 0) else exchange(piece(last, j, c), 2) for j in range(rows)]
        for c in range(chunks)
    ]
    zs = [[forward(ys[c][j]) for j in range(DEPTH)] for c in range(chunks)]
    side_cond = exchange(inner(cond_own), 1)
    sides = exchange(strips, 1)

    zero_side = jnp.zeros_like(side_cond)
    blank = jnp.zeros((deep, PAD - HALO), jnp.float32)
    cond = jnp.concatenate(
        [
            blank,
            jnp.where(block_col == 1, side_cond, zero_side),
            cond_own,
            jnp.where(block_col == 0, side_cond, zero_side),
            blank,
        ],
        1,
    )
    has_z = jnp.where(flip == 0, me >= 4, me < count - 4)
    level = jnp.arange(deep)[:, None]
    next_row = jnp.concatenate([cond[1:], jnp.zeros((1, wide), jnp.float32)], 0)
    next_col = jnp.concatenate([cond[:, 1:], jnp.zeros((deep, 1), jnp.float32)], 1)
    ws = jnp.where(has_z | (level >= DEPTH), 0.5 * (cond + next_row), 0.0)
    low = jnp.where(block_col == 0, PAD, HALO)
    high = jnp.where(block_col == 0, wide - HALO, wide - PAD)
    spot = jnp.arange(wide)[None, :]
    we = jnp.where((spot >= low) & (spot + 1 < high), 0.5 * (cond + next_col), 0.0)
    ws = jnp.broadcast_to(ws[:, :, None], (deep, wide, LANES))
    we = jnp.broadcast_to(we[:, :, None], (deep, wide, LANES))
    left = jnp.where(block_col == 1, sides, 0.0)
    right = jnp.where(block_col == 0, sides, 0.0)

    def located(cell):
        row = cell // (2 * cols) - block_row * rows + DEPTH
        row = jnp.where(flip == 0, row, deep - 1 - row)
        col = cell % (2 * cols) - block_col * cols + PAD
        inside = (row >= 0) & (row < deep) & (col >= HALO) & (col < wide - HALO)
        return jnp.where(inside, row * wide + col, -1)[None, :]

    src = located(source_cell)
    gnd = located(ground_cell)
    flag = flip.astype(jnp.int32)[None]

    fields = None
    sums = []
    for c in range(chunks):
        *fields, part = krylov(
            c, flag, own, ys[c], zs[c], left, right, ws, we, src, gnd, fields
        )
        sums.append(part)
    rr, rw, ww, wz, xd, rd, wd, _ = total(jnp.concatenate(sums, 1))
    a0 = rr / rw
    rr1 = rr + a0 * (a0 * ww - 2.0 * rw)
    grow = 1.0 + rr1 / rr
    curve = grow * (grow * rw - 2.0 * a0 * ww) + a0 * a0 * wz
    a1 = rr1 / curve
    p = a0 + a1 * grow
    q = a0 * a1
    r, w, z = fields
    potentials = own + p * r - q * w
    residual = r - p * w + q * z
    return (potentials[None], residual[None], xd + p * rd - q * wd)


def solution(mesh):
    placed = (
        P(("grp", "tile"), None, None),
        P(),
        P("grp"),
        P("grp"),
        P(("grp", "tile"), None, None, None),
    )
    return jax.shard_map(
        shards,
        mesh=mesh,
        in_specs=placed,
        out_specs=(
            P(("grp", "tile"), None, None, None),
            P(("grp", "tile"), None, None, None),
            P("grp"),
        ),
        check_vma=False,
    )
```
